32 devices in a mesh: dp: 1 (over z), c: 4 (over y), r: 8 (over x, core).
Axes of the slice: x: 4, y: 4, z: 1, core: 2. Of those that a mesh axis runs over, the one named last changes fastest.
The devices are a block of a 4x4x8 slice.
Arguments:
- x: bfloat16 [6144, 3584], P(('dp', 'r'), 'c')
- w: bfloat16 [3584, 28672], P('r', 'c')
- dy: bfloat16 [6144, 28672], P(('dp', 'r'), 'c')
Outputs:
- output 1: bfloat16 [6144, 3584], P(('dp', 'r'), 'c')
- output 2: float32 [3584, 28672], P(('dp', 'r'), 'c')
All inputs are finite; a program needn't handle non-finite values.
Results may differ from the reference program's by a relative error of at most 0.001.
Values are sent between devices in bfloat16 or wider.
A program may use at most 768 MiB of HBM per device.

```python
import jax
import jax.numpy as jnp

T = 6144
H = 3584
F = 14336


def setup_inputs(seed: int = 0, part: int = 0) -> dict:
    base = jax.random.PRNGKey(seed)
    kw, kpart = jax.random.split(base)
    kx, kdy = jax.random.split(jax.random.fold_in(kpart, part))
    n = 2 * F
    x = jax.random.normal(kx, (T, H), jnp.float32)
    w = jax.random.normal(kw, (H, n), jnp.float32) * H ** -0.5
    dy = jax.random.normal(kdy, (T, n), jnp.float32) * (T * n / H) ** -0.25
    return {"x": x.astype(jnp.bfloat16), "w": w.astype(jnp.bfloat16), "dy": dy.astype(jnp.bfloat16)}


def reference(x, w, dy):
    dx = jnp.dot(dy, w.T, preferred_element_type=jnp.float32).astype(jnp.bfloat16)
    dw = jnp.dot(x.T, dy, preferred_element_type=jnp.float32)
    return dx, dw
```

```python
import functools

import jax
import jax.numpy as jnp
from jax import lax
from jax.experimental import pallas as pl
from jax.experimental.pallas import tpu as pltpu
from jax.sharding import PartitionSpec as P

MESH = pl.DeviceIdType.MESH
ROWS = 128
TILE = 1024


def _kernel(nr, nc, x, w, dy, dx, dw, dyg,
            dyb, wv, dwv, xin, xts, x0, xt, pb, rb, st, dxb, dxo,
            sr, sl, ss, fr, fl, fs, qr, ql, qs, qor, qol, qso,
            sx0, rx0, sx1, rx1, sx2, rx2, sp, rp, sd, rd, lsem):
    r = lax.axis_index("r")
    j = lax.axis_index("c")
    i, k = r // 2, lax.rem(r, 2)
    tb, kb = x.shape
    kd, nb = w.shape
    kq = kd // nc
    ncomm = tb // ROWS
    half = nb // 2
    big = 2 * ROWS

    def rot(d):
        return lax.rem(r + d + nr, nr)

    right, left, opp = rot(2), rot(-2), rot(nr // 2)
    sib = r + 1 - 2 * k
    sibright, sibleft, sibopp = lax.rem(sib + 2, nr), lax.rem(sib - 2 + nr, nr), lax.rem(sib + nr // 2, nr)

    def remote(src, dst, s, q, **dev):
        return pltpu.make_async_remote_copy(src_ref=src, dst_ref=dst, send_sem=s, recv_sem=q,
                                            device_id=dev, device_id_type=MESH)

    def rows(c, n=ROWS):
        return pl.ds(pl.multiple_of(c * n, n), n)

    load_x = pltpu.make_async_copy(x, xin, lsem.at[0])
    load_w = pltpu.make_async_copy(w, wv, lsem.at[1])
    load_x.start()
    load_w.start()
    bar = pltpu.get_barrier_semaphore()
    for dc in range(nc):
        for dr in range(nr):
            if dc or dr:
                pl.semaphore_signal(bar, inc=1, device_id={"c": lax.rem(j + dc, nc), "r": lax.rem(r + dr, nr)},
                                    device_id_type=MESH)
    pl.semaphore_wait(bar, nc * nr - 1)

    def own_right(c):
        return remote(dy.at[rows(c)], dyg.at[r, rows(c)], sr.at[c], ql.at[c], r=right)

    def own_left(c):
        return remote(dy.at[rows(c)], dyg.at[r, rows(c)], sl.at[c], qr.at[c], r=left)

    def to_sib(blk, kind, c):
        src = dy.at[rows(c)] if kind == 0 else dyg.at[blk, rows(c)]
        return remote(src, dyg.at[blk, rows(c)], ss.at[kind, c], qs.at[kind, c], r=sib)

    def fwd_right(c):
        return remote(dyg.at[left, rows(c), pl.ds(0, half)], dyg.at[left, rows(c), pl.ds(0, half)],
                      fr.at[c], qol.at[c], r=right)

    def fwd_left(c):
        return remote(dyg.at[right, rows(c), pl.ds(half, half)], dyg.at[right, rows(c), pl.ds(half, half)],
                      fl.at[c], qor.at[c], r=left)

    def opp_sib(h, c):
        return remote(dyg.at[opp, rows(c), pl.ds(h * half, half)], dyg.at[opp, rows(c), pl.ds(h * half, half)],
                      fs.at[h, c], qso.at[h, c], r=sib)

    own_right(0).start()
    own_left(0).start()

    load_x.wait()
    xts[...] = xin[...].T
    for kk in range(2):
        x0[j, kk] = xts[pl.ds(pl.multiple_of(kk * kd + j * kq, 16), kq)]

    def x_spread(dq, kk):
        q = lax.rem(j + dq, nc)
        return remote(xts.at[pl.ds(pl.multiple_of(kk * kd + q * kq, 16), kq)], x0.at[j, kk],
                      sx0.at[dq - 1, kk], rx0.at[dq - 1, kk], c=q)

    def x_cross(d):
        t = lax.rem(r + d, nr)
        return remote(x0.at[t // 2, lax.rem(t, 2)], xt.at[r, pl.ds(pl.multiple_of(j * kq, 16), kq)],
                      sx1.at[d - 1], rx1.at[d - 1], r=t)

    def x_gather(dq):
        mine = xt.at[:, pl.ds(pl.multiple_of(j * kq, 16), kq)]
        return remote(mine, mine, sx2.at[dq - 1], rx2.at[dq - 1], c=lax.rem(j + dq, nc))

    for dq in range(1, nc):
        for kk in range(2):
            x_spread(dq, kk).start()

    def zero(t, _):
        dwv[:, pl.ds(pl.multiple_of(t * TILE, TILE), TILE)] = jnp.zeros((kd, TILE), jnp.float32)
        return 0

    lax.fori_loop(0, nb // TILE, zero, 0)
    for dq in range(1, nc):
        for kk in range(2):
            x_spread(dq, kk).wait_recv()
    for d in range(1, nr):
        x_cross(d).start()
    xt[r, pl.ds(pl.multiple_of(j * kq, 16), kq)] = x0[i, k]
    for c in range(ncomm):
        if c:
            own_right(c).start()
            own_left(c).start()
        to_sib(r, 0, c).start()
    for d in range(1, nr):
        x_cross(d).wait_recv()
    for dq in range(1, nc):
        x_gather(dq).start()
    load_w.wait()
    for dq in range(1, nc):
        x_gather(dq).wait_recv()

    def exchange(s, base, n, ps, dq):
        q = lax.rem(j + dq, nc)
        return remote(pb.at[ps, pl.ds(pl.multiple_of(q * n, n), n)], rb.at[dq - 1, pl.ds(pl.multiple_of(base, n), n)],
                      sp.at[dq - 1, ps], rp.at[dq - 1, s], c=q)

    def owner(blk, off, base, n, own):
        return remote(st.at[pl.ds(pl.multiple_of(base, n), n)],
                      dxb.at[k, pl.ds(pl.multiple_of(off + j * n, n), n)],
                      sd.at[own], rd.at[k, j], c=i, r=blk)

    def reduce(s, blk, off, base, n, ps):
        for dq in range(1, nc):
            exchange(s, base, n, ps, dq).wait_recv()
        total = pb[ps, pl.ds(pl.multiple_of(j * n, n), n)]
        at = pl.ds(pl.multiple_of(base, n), n)
        for dq in range(1, nc):
            total += rb[dq - 1, at]
        st[at] = total.astype(jnp.bfloat16)

    def deliver(blk, off, base, n):
        @pl.when(blk != r)
        def _():
            owner(blk, off, base, n, 1).start()

        @pl.when((blk == r) & (i != j))
        def _():
            owner(blk, off, base, n, 0).start()

        @pl.when((blk == r) & (i == j))
        def _():
            dxb[k, pl.ds(pl.multiple_of(off + j * n, n), n)] = st[pl.ds(pl.multiple_of(base, n), n)]

    def step(s, blk, off, base, n, slot, local, prev, sent):
        m = n * nc
        at = pl.ds(pl.multiple_of(off, m), m)
        buf = dyb.at[slot, pl.ds(0, m)]

        @pl.when(local)
        def _():
            pltpu.make_async_copy(dy.at[at], buf, lsem.at[2]).start()

        @pl.when(jnp.logical_not(local))
        def _():
            pltpu.make_async_copy(dyg.at[blk, at], buf, lsem.at[2]).start()

        @pl.when(sent)
        def _():
            for dq in range(1, nc):
                exchange(s, base, n, slot, dq).wait_send()

        if prev is not None:
            @pl.when(prev[0])
            def _():
                reduce(*prev[1:])
        pltpu.make_async_copy(dy.at[pl.ds(0, m)], buf, lsem.at[2]).wait()

        pb[slot, pl.ds(0, m)] = jnp.zeros((m, kd), jnp.float32)

        def dx_tile(t, _):
            cols = pl.ds(pl.multiple_of(t * TILE, TILE), TILE)
            pb[slot, pl.ds(0, m)] += lax.dot_general(dyb[slot, pl.ds(0, m), cols], wv[:, cols], (((1,), (1,)), ((), ())),
                                                     preferred_element_type=jnp.float32)
            return 0

        lax.fori_loop(0, nb // TILE, dx_tile, 0)
        if prev is not None:
            @pl.when(prev[0])
            def _():
                deliver(*prev[2:6])

        def dw_tile(t, _):
            cols = pl.ds(pl.multiple_of(t * TILE, TILE), TILE)
            dwv[:, cols] += jnp.dot(xt[blk, :, at], dyb[slot, pl.ds(0, m), cols], preferred_element_type=jnp.float32)
            return 0

        lax.fori_loop(0, 1, dw_tile, 0)
        for dq in range(1, nc):
            exchange(s, base, n, slot, dq).start()
        lax.fori_loop(1, nb // TILE, dw_tile, 0)

    n1, n2 = big // nc, ROWS // nc
    nbig = tb // big
    steps1 = 6 * nbig
    steps2 = 2 * ncomm

    def where1(s):
        t = s - 2 * nbig
        kind = lax.rem(t, 4)
        blk = jnp.where(s < nbig, r, jnp.where(s < 2 * nbig, sib, jnp.where(
            kind == 0, left, jnp.where(kind == 1, right, jnp.where(kind == 2, sibleft, sibright)))))
        c = jnp.where(s < 2 * nbig, lax.rem(s, nbig), t // 4)
        return blk, c

    def body1(s, _):
        t = s - 2 * nbig
        kind = lax.rem(t, 4)
        blk, c = where1(s)

        @pl.when((s >= nbig) & (s < 2 * nbig))
        def _():
            for h in range(2):
                to_sib(sib, 0, 2 * c + h).wait_recv()

        @pl.when((s >= 2 * nbig) & (kind == 0))
        def _():
            for h in range(2):
                own_right(2 * c + h).wait_recv()
                fwd_right(2 * c + h).start()
                to_sib(left, 1, 2 * c + h).start()

        @pl.when((s >= 2 * nbig) & (kind == 1))
        def _():
            for h in range(2):
                own_left(2 * c + h).wait_recv()
                fwd_left(2 * c + h).start()
                to_sib(right, 2, 2 * c + h).start()

        @pl.when((s >= 2 * nbig) & (kind == 2))
        def _():
            for h in range(2):
                to_sib(sibleft, 1, 2 * c + h).wait_recv()

        @pl.when((s >= 2 * nbig) & (kind == 3))
        def _():
            for h in range(2):
                to_sib(sibright, 2, 2 * c + h).wait_recv()

        pblk, pc = where1(s - 1)
        step(s, blk, c * big, s * n1, n1, lax.rem(s, 2), s < nbig,
             (s > 0, s - 1, pblk, pc * big, (s - 1) * n1, n1, lax.rem(s + 1, 2)), s >= 2)
        return 0

    lax.fori_loop(0, steps1, body1, 0)
    last = steps1 - 1
    blk, c = where1(last)
    reduce(last, blk, c * big, last * n1, n1, last % 2)
    for ps in range(2):
        for dq in range(1, nc):
            exchange(0, 0, n1, ps, dq).wait_send()
    base2 = steps1 * n1

    def where2(t):
        return jnp.where(lax.rem(t, 2) == 0, opp, sibopp), t // 2

    def body2(t, _):
        blk, c = where2(t)

        @pl.when(lax.rem(t, 2) == 0)
        def _():
            fwd_right(c).wait_recv()
            opp_sib(0, c).start()
            fwd_left(c).wait_recv()
            opp_sib(1, c).start()

        @pl.when(lax.rem(t, 2) == 1)
        def _():
            for h in range(2):
                opp_sib(h, c).wait_recv()

        @pl.when(t == 0)
        def _():
            pblk, pc = where1(last)
            deliver(pblk, pc * big, last * n1, n1)

        pblk, pc = where2(t - 1)
        step(steps1 + t, blk, c * ROWS, base2 + t * n2, n2, lax.rem(t, 2), t < 0,
             (t > 0, steps1 + t - 1, pblk, pc * ROWS, base2 + (t - 1) * n2, n2, lax.rem(t + 1, 2)), t >= 2)
        return 0

    lax.fori_loop(0, steps2, body2, 0)
    end = steps2 - 1
    blk, c = where2(end)

    def flush(t):
        cols = pl.ds(t * TILE, TILE)
        return pltpu.make_async_copy(dwv.at[:, cols], dw.at[:, cols], lsem.at[3 + t])

    for t in range(nb // TILE):
        flush(t).start()
    reduce(steps1 + end, blk, c * ROWS, base2 + end * n2, n2, end % 2)
    deliver(blk, c * ROWS, base2 + end * n2, n2)

    piece = tb // nc
    for kk in range(2):
        for q in range(nc):
            @pl.when(jnp.logical_not((i == j) & (k == kk) & (j == q)))
            def _():
                remote(st.at[pl.ds(0, piece)], dxb.at[kk, pl.ds(0, piece)], sd.at[0], rd.at[kk, q], c=i, r=sib).wait_recv()
    dxo[:, :kd] = dxb[0]
    dxo[:, kd:] = dxb[1]
    put = pltpu.make_async_copy(dxo, dx, lsem.at[0])
    put.start()

    for ps in range(2):
        for dq in range(1, nc):
            exchange(0, 0, n2, ps, dq).wait_send()

    @pl.when(i != j)
    def _():
        remote(st.at[pl.ds(0, piece)], dxb.at[0, pl.ds(0, piece)], sd.at[0], rd.at[0, 0], c=i, r=sib).wait_send()

    others = (nr - 1) * piece
    remote(st.at[pl.ds(0, others)], st.at[pl.ds(0, others)], sd.at[1], rd.at[0, 0], c=i, r=sib).wait_send()
    for c in range(ncomm):
        own_right(c).wait_send()
        own_left(c).wait_send()
        fwd_right(c).wait_send()
        fwd_left(c).wait_send()
        for kind in range(3):
            to_sib(r, kind, c).wait_send()
        for h in range(2):
            opp_sib(h, c).wait_send()
    for dq in range(1, nc):
        for kk in range(2):
            x_spread(dq, kk).wait_send()
        x_gather(dq).wait_send()
    for d in range(1, nr):
        x_cross(d).wait_send()
    for t in range(nb // TILE):
        flush(t).wait()
    put.wait()


def solution(mesh):
    nr, nc = mesh.shape["r"], mesh.shape["c"]

    def local(x, w, dy):
        tb, kb = x.shape
        kd, nb = w.shape
        ncomm = tb // ROWS
        big = 2 * ROWS
        nsteps = 6 * (tb // big) + 2 * ncomm
        bf16, f32 = jnp.bfloat16, jnp.float32
        dma = pltpu.SemaphoreType.DMA
        any_ = pl.BlockSpec(memory_space=pl.ANY)
        out = pl.pallas_call(
            functools.partial(_kernel, nr, nc),
            name="linear_backward",
            out_shape=(jax.ShapeDtypeStruct((tb, kb), bf16), jax.ShapeDtypeStruct((kd, nb), f32),
                       jax.ShapeDtypeStruct((nr, tb, nb), bf16)),
            in_specs=[any_] * 3,
            out_specs=(any_,) * 3,
            scratch_shapes=[
                pltpu.VMEM((2, big, nb), bf16), pltpu.VMEM((kd, nb), bf16), pltpu.VMEM((kd, nb), f32),
                pltpu.VMEM((tb, kb), bf16), pltpu.VMEM((kb, tb), bf16), pltpu.VMEM((nc, 2, kd // nc, tb), bf16),
                pltpu.VMEM((nr, kd, tb), bf16), pltpu.VMEM((2, big, kd), f32),
                pltpu.VMEM((nc - 1, nr * tb // nc, kd), f32), pltpu.VMEM((nr * tb // nc, kd), bf16),
                pltpu.VMEM((2, tb, kd), bf16), pltpu.VMEM((tb, kb), bf16),
                dma((ncomm,)), dma((ncomm,)), dma((3, ncomm)), dma((ncomm,)), dma((ncomm,)), dma((2, ncomm)),
                dma((ncomm,)), dma((ncomm,)), dma((3, ncomm)), dma((ncomm,)), dma((ncomm,)), dma((2, ncomm)),
                dma((nc - 1, 2)), dma((nc - 1, 2)), dma((nr - 1,)), dma((nr - 1,)), dma((nc - 1,)), dma((nc - 1,)),
                dma((nc - 1, 2)), dma((nc - 1, nsteps)), dma((2,)), dma((2, nc)), dma((3 + nb // TILE,)),
            ],
            compiler_params=pltpu.CompilerParams(collective_id=0, has_side_effects=True,
                                                 vmem_limit_bytes=67043328),
        )(x, w, dy)
        return out[0], out[1]

    act = P(("dp", "r"), "c")
    return jax.shard_map(local, mesh=mesh, in_specs=(act, P("r", "c"), act),
                         out_specs=(act, act), check_vma=False)
```

```python
import functools

import jax
import jax.numpy as jnp
from jax import lax
from jax.experimental import pallas as pl
from jax.experimental.pallas import tpu as pltpu
from jax.sharding import PartitionSpec as P

MESH = pl.DeviceIdType.MESH
ROWS = 128
FIRST = 3
SUB = 64
TILE = 1024
VMEM = 67043328
PUTS = 4


def _main(nr, nc, x, w, dy, dwv, dxb, dxl, dyg,
          dyb, dyl, wv, xin, xts, x0, xt, pb, pt, rb, rt, st, stl,
          s_own, s_fwd, s_sib, s_opp, q_left, q_right, q_sib, q_fwd, q_opp, s_last, q_last, q_slast,
          s_x, q_x, s_part, q_part, s_dx, q_dx, q_dxl, lsem):
    r = lax.axis_index("r")
    j = lax.axis_index("c")
    i, k = r // 2, lax.rem(r, 2)
    tb = x.shape[0]
    kd, nb = w.shape
    kq = kd // nc
    half = nb // 2
    m = 2 * ROWS
    nbig = tb // m
    early = 6 * nbig
    runs = tb // ROWS - 1
    steps = early + runs
    subs = ROWS // SUB

    def rot(d):
        return lax.rem(r + d + nr, nr)

    right, left, opp = rot(2), rot(-2), rot(nr // 2)
    sib = r + 1 - 2 * k
    sibright, sibleft, sibopp = lax.rem(sib + 2, nr), lax.rem(sib - 2 + nr, nr), lax.rem(sib + nr // 2, nr)

    def remote(src, dst, s, q, **dev):
        return pltpu.make_async_remote_copy(src_ref=src, dst_ref=dst, send_sem=s, recv_sem=q,
                                            device_id=dev, device_id_type=MESH)

    def at(start, size):
        return pl.ds(pl.multiple_of(start, size), size)

    load_x = pltpu.make_async_copy(x, xin, lsem.at[0])
    load_w = pltpu.make_async_copy(w, wv, lsem.at[1])
    load_x.start()
    load_w.start()
    bar = pltpu.get_barrier_semaphore()
    for dc in range(nc):
        for dr in range(nr):
            if dc or dr:
                pl.semaphore_signal(bar, inc=1, device_id={"c": lax.rem(j + dc, nc), "r": lax.rem(r + dr, nr)},
                                    device_id_type=MESH)
    pl.semaphore_wait(bar, nc * nr - 1)

    def own_right(row, size):
        rows = pl.ds(row, size)
        return remote(dy.at[rows], dyg.at[r, rows], s_own.at[0], q_left.at[row // m], r=right)

    def own_left(row, size):
        rows = pl.ds(row, size)
        return remote(dy.at[rows], dyg.at[r, rows], s_own.at[1], q_right.at[row // m], r=left)

    def to_sib(blk, kind, c):
        src = dy.at[at(c * m, m)] if kind == 0 else dyg.at[blk, at(c * m, m)]
        return remote(src, dyg.at[blk, at(c * m, m)], s_sib.at[kind], q_sib.at[kind, c], r=sib)

    def wait_left(c):
        remote(dy.at[at(c * m, m)], dyg.at[left, at(c * m, m)], s_own.at[0], q_left.at[c], r=right).wait_recv()

    def wait_right(c):
        remote(dy.at[at(c * m, m)], dyg.at[right, at(c * m, m)], s_own.at[1], q_right.at[c], r=left).wait_recv()

    def part(blk, h, row, size):
        return dyg.at[blk, at(row, size), pl.ds(h * half, half)]

    def forward(h, row, size, q):
        blk, to = ((left, right), (right, left))[h]
        return remote(part(blk, h, row, size), part(blk, h, row, size), s_fwd.at[h], q_fwd.at[h, q], r=to)

    def opp_in(h, row, size, q):
        return remote(part(opp, h, row, size), part(opp, h, row, size), s_fwd.at[h], q_fwd.at[h, q], r=right)

    def opp_sib(h, row, size, q):
        return remote(part(opp, h, row, size), part(opp, h, row, size), s_opp, q_opp.at[q], r=sib)

    def wait_opp_sib(row, size, q):
        rows = dyg.at[sibopp, at(row, size)]
        remote(rows, rows, s_opp, q_opp.at[q], r=sib).wait_recv()

    def last(h, u, row):
        return dyl.at[pl.ds(pl.multiple_of(row + u * SUB, SUB), SUB), pl.ds(h * half, half)]

    def forward_last(h, u):
        blk, to = ((left, right), (right, left))[h]
        return remote(part(blk, h, tb - ROWS + u * SUB, SUB), last(h, u, 0), s_fwd.at[h], q_last.at[h, u], r=to)

    def sib_last(h, u):
        return remote(last(h, u, 0), last(h, u, ROWS), s_last, q_slast.at[u], r=sib)

    own_right(0, ROWS).start()
    own_left(0, ROWS).start()

    load_x.wait()
    xts[...] = xin[...].T
    for kk in range(2):
        x0[j, kk] = xts[pl.ds(pl.multiple_of(kk * kd + j * kq, 16), kq)]
    mine = pl.ds(pl.multiple_of(j * kq, 16), kq)

    for dq in range(1, nc):
        for kk in range(2):
            q = lax.rem(j + dq, nc)
            remote(xts.at[pl.ds(pl.multiple_of(kk * kd + q * kq, 16), kq)], x0.at[j, kk],
                   s_x.at[0], q_x.at[0], c=q).start()
    spread = remote(x0.at[pl.ds(0, nc - 1)], x0.at[pl.ds(0, nc - 1)], s_x.at[0], q_x.at[0], c=lax.rem(j + 1, nc))

    def zero(t, _):
        dwv[:, at(t * TILE, TILE)] = jnp.zeros((kd, TILE), jnp.float32)
        return 0

    lax.fori_loop(0, nb // TILE, zero, 0)
    with jax.named_scope("xspread"):
        spread.wait_recv()
    for d in range(1, nr):
        t = lax.rem(r + d, nr)
        remote(x0.at[t // 2, lax.rem(t, 2)], xt.at[r, mine], s_x.at[1], q_x.at[1], r=t).start()
    cross = remote(xt.at[pl.ds(0, nr - 1), mine], xt.at[pl.ds(0, nr - 1), mine], s_x.at[1], q_x.at[1], r=right)
    xt[r, mine] = x0[i, k]
    own_right(ROWS, ROWS).start()
    own_left(ROWS, ROWS).start()
    to_sib(r, 0, 0).start()
    for c in range(1, nbig):
        own_right(c * m, m).start()
        own_left(c * m, m).start()
        to_sib(r, 0, c).start()
    with jax.named_scope("xcross"):
        cross.wait_recv()
    for dq in range(1, nc):
        remote(xt.at[:, mine], xt.at[:, mine], s_x.at[2], q_x.at[2], c=lax.rem(j + dq, nc)).start()
    others = pl.ds(0, (nc - 1) * kq)
    gather = remote(xt.at[:, others], xt.at[:, others], s_x.at[2], q_x.at[2], c=lax.rem(j + 1, nc))
    load_w.wait()

    def where(s):
        t = s - 2 * nbig
        kind = lax.rem(t, 4)
        late = s >= early
        blk = jnp.where(s < nbig, r, jnp.where(s < 2 * nbig, sib, jnp.where(
            kind == 0, left, jnp.where(kind == 1, right, jnp.where(kind == 2, sibleft, sibright)))))
        c = 2 * jnp.where(s < 2 * nbig, lax.rem(s, nbig), t // 4)
        blka = jnp.where(late, opp, blk)
        blkb = jnp.where(late, sibopp, blk)
        ca = jnp.where(late, s - early, c)
        cb = jnp.where(late, s - early, c + 1)
        return blka, ca, blkb, cb

    def fetch(src, blk, row, size, slot, to, h):
        rows = src.at[at(row, size)] if blk is None else src.at[blk, at(row, size)]
        return pltpu.make_async_copy(rows, dyb.at[slot, pl.ds(to, size)], lsem.at[2 + h])

    def arrive(s):
        blka, ca, blkb, cb = where(s)
        slot = lax.rem(s, 2)
        t = s - 2 * nbig
        kind = lax.rem(t, 4)
        c = t // 4
        mid = (s >= 2 * nbig) & (s < early)

        @pl.when((s >= nbig) & (s < 2 * nbig))
        def _():
            to_sib(sib, 0, s - nbig).wait_recv()

        for h in range(2):
            @pl.when(mid & (kind == h))
            def _():
                (wait_left, wait_right)[h](c)

                forward(h, 2 * c * ROWS, ROWS, 2 * c).start()

                @pl.when(c < nbig - 1)
                def _():
                    forward(h, (2 * c + 1) * ROWS, ROWS, 2 * c + 1).start()

                @pl.when(c == nbig - 1)
                def _():
                    for u in range(subs):
                        forward_last(h, u).start()

                to_sib((left, right)[h], 1 + h, c).start()

            @pl.when(mid & (kind == 2 + h))
            def _():
                to_sib((sibleft, sibright)[h], 1 + h, c).wait_recv()

        @pl.when(s < nbig)
        def _():
            fetch(dy, None, ca * ROWS, ROWS, slot, 0, 0).start()
            fetch(dy, None, cb * ROWS, ROWS, slot, ROWS, 1).start()

        @pl.when(s >= nbig)
        def _():
            @pl.when(s >= early)
            def _():
                with jax.named_scope("opp"):
                    for h in range(2):
                        opp_in(h, ca * ROWS, ROWS, ca).wait_recv()
                        opp_sib(h, ca * ROWS, ROWS, ca).start()

            fetch(dyg, blka, ca * ROWS, ROWS, slot, 0, 0).start()

            @pl.when(s >= early)
            def _():
                with jax.named_scope("oppsib"):
                    wait_opp_sib(ca * ROWS, ROWS, ca)

            fetch(dyg, blkb, cb * ROWS, ROWS, slot, ROWS, 1).start()

    def exchange(s):
        ps = lax.rem(s, 3)
        for dq in range(1, nc):
            q = lax.rem(j + dq, nc)
            remote(pb.at[ps, pl.ds(pl.multiple_of(q * kq, 16), kq)], rb.at[dq - 1, s], s_part.at[ps], q_part.at[s], c=q).start()

    def exchanged(s):
        ps = lax.rem(s, 3)
        rows = pl.ds(0, (nc - 1) * kq)
        return remote(pb.at[ps, rows], pb.at[ps, rows], s_part.at[ps], q_part.at[s], c=lax.rem(j + 1, nc))

    def sum_step(s):
        exchanged(s).wait_recv()
        acc = pb[lax.rem(s, 3), mine]
        for dq in range(1, nc):
            acc += rb[dq - 1, s]
        st[s] = acc.astype(jnp.bfloat16)

    def send_dx(s, lanes, blk, row, size):
        src = st.at[s, :, lanes]
        share = pl.ds(pl.multiple_of(k * kd + j * kq, 16), kq)
        dst = dxb.at[share, at(row, size)]

        @pl.when(blk != r)
        def _():
            remote(src, dst, s_dx.at[1], q_dx.at[k], c=i, r=blk).start()

        @pl.when((blk == r) & (i != j))
        def _():
            remote(src, dst, s_dx.at[0], q_dx.at[k], c=i, r=blk).start()

        @pl.when((blk == r) & (i == j))
        def _():
            dxb[share, at(row, size)] = st[s, :, lanes]

    def deliver_early(s):
        blka, ca, _, _ = where(s)
        send_dx(s, pl.ds(0, m), blka, ca * ROWS, m)

    def deliver_late(s):
        blka, ca, blkb, cb = where(s)
        send_dx(s, pl.ds(0, ROWS), blka, ca * ROWS, ROWS)
        send_dx(s, pl.ds(ROWS, ROWS), blkb, cb * ROWS, ROWS)

    def exchange_last(u):
        for dq in range(1, nc):
            q = lax.rem(j + dq, nc)
            remote(pt.at[u, pl.ds(pl.multiple_of(q * kq, 16), kq)], rt.at[dq - 1, u], s_part.at[3 + u], q_part.at[steps + u],
                   c=q).start()

    def exchanged_last(u):
        rows = pl.ds(0, (nc - 1) * kq)
        return remote(pt.at[u, rows], pt.at[u, rows], s_part.at[3 + u], q_part.at[steps + u], c=lax.rem(j + 1, nc))

    def sum_last(u):
        exchanged_last(u).wait_recv()
        acc = pt[u, mine]
        for dq in range(1, nc):
            acc += rt[dq - 1, u]
        stl[u] = acc.astype(jnp.bfloat16)

    def deliver_last(u):
        share = pl.ds(pl.multiple_of(k * kd + j * kq, 16), kq)
        for blk in (opp, sibopp):
            remote(stl.at[u], dxl.at[share, at(u * 2 * SUB, 2 * SUB)], s_dx.at[1], q_dxl.at[k], c=i, r=blk).start()

    arrive(jnp.int32(0))
    with jax.named_scope("xgather"):
        gather.wait_recv()

    def dw_tiles(buf, blka, ca, blkb, cb, lo, hi):
        def dw_tile(t, _):
            cols = at(t * TILE, TILE)
            lhs = jnp.concatenate([xt[blka, :, at(ca * ROWS, ROWS)], xt[blkb, :, at(cb * ROWS, ROWS)]], axis=1)
            dwv[:, cols] += jnp.dot(lhs, buf[:, cols], preferred_element_type=jnp.float32)
            return 0

        lax.fori_loop(lo, hi, dw_tile, 0)

    def step(s, _):
        slot, ps = lax.rem(s, 2), lax.rem(s, 3)
        blka, ca, blkb, cb = where(s)

        @pl.when(s >= 3)
        def _():
            exchanged(s - 3).wait_send()

        with jax.named_scope("reduce"):
            @pl.when((s >= 2) & (s <= early))
            def _():
                sum_step(s - 2)

            @pl.when(s >= early)
            def _():
                sum_step(s - 1)

        with jax.named_scope("loadwait"):
            for h in range(2):
                fetch(dyg, r, 0, ROWS, slot, h * ROWS, h).wait()
        pb[ps] = jnp.zeros((kd, m), jnp.float32)

        def dx_tile(t, _):
            cols = at(t * TILE, TILE)
            pb[ps] += lax.dot_general(wv[:, cols], dyb[slot, :, cols], (((1,), (1,)), ((), ())),
                                      preferred_element_type=jnp.float32)
            return 0

        with jax.named_scope("dx"):
            lax.fori_loop(0, nb // TILE, dx_tile, 0)

        dw_tiles(dyb.at[slot], blka, ca, blkb, cb, 0, 1)
        exchange(s)

        @pl.when((s >= 2) & (s < FIRST + 2))
        def _():
            deliver_early(s - 2)

        per = -(-(early - FIRST) // runs)
        for d in range(per):
            old = FIRST + (s - early) * per + d

            @pl.when((s >= early) & (old < early))
            def _():
                deliver_early(old)

        @pl.when(s > early)
        def _():
            deliver_late(s - 1)

        @pl.when(s < early - 1)
        def _():
            arrive(s + 1)

        with jax.named_scope("dw"):
            dw_tiles(dyb.at[slot], blka, ca, blkb, cb, 1, nb // TILE)

        @pl.when((s >= early - 1) & (s < steps - 1))
        def _():
            arrive(s + 1)

        return 0

    lax.fori_loop(0, steps, step, 0)

    for u in range(subs):
        with jax.named_scope("opp"):
            for h in range(2):
                forward_last(h, u).wait_recv()
                sib_last(h, u).start()
        if u == 0:
            pt[...] = jnp.zeros((subs, kd, 2 * SUB), jnp.float32)
        with jax.named_scope("oppsib"):
            both = dyl.at[pl.ds(0, SUB)]
            remote(both, both, s_last, q_slast.at[u], r=sib).wait_recv()

        def dx_tile(t, _):
            cols = at(t * TILE, TILE)
            rhs = jnp.concatenate([dyl[pl.ds(u * SUB, SUB), cols], dyl[pl.ds(ROWS + u * SUB, SUB), cols]], axis=0)
            pt[u] += lax.dot_general(wv[:, cols], rhs, (((1,), (1,)), ((), ())), preferred_element_type=jnp.float32)
            return 0

        with jax.named_scope("dx"):
            lax.fori_loop(0, nb // TILE, dx_tile, 0)
        if u == subs - 1:
            dw_tiles(dyl, opp, runs, sibopp, runs, 0, 1)
        exchange_last(u)
        if u == 0:
            with jax.named_scope("reduce"):
                sum_step(steps - 1)

    deliver_late(steps - 1)
    with jax.named_scope("dw"):
        dw_tiles(dyl, opp, runs, sibopp, runs, 1, nb // TILE)
    for u in range(subs - 1):
        with jax.named_scope("reduce"):
            sum_last(u)
        deliver_last(u)

    for d in range(2):
        remote(dy, dyg.at[r], s_own.at[d], q_left.at[0], r=right).wait_send()
        remote(dyg.at[r, :, pl.ds(0, half)], dyg.at[r, :, pl.ds(0, half)], s_fwd.at[d], q_left.at[0], r=right).wait_send()
    for kind in range(3):
        remote(dy, dyg.at[r], s_sib.at[kind], q_left.at[0], r=right).wait_send()
    sent = dyg.at[r, pl.ds(0, runs * ROWS)]
    remote(sent, sent, s_opp, q_left.at[0], r=right).wait_send()
    sent = dyl.at[pl.ds(0, ROWS)]
    remote(sent, sent, s_last, q_left.at[0], r=right).wait_send()
    for sent in (spread, cross, gather):
        sent.wait_send()
    for s in range(steps - 3, steps):
        exchanged(s).wait_send()
    with jax.named_scope("reduce"):
        sum_last(subs - 1)
    for u in range(subs):
        exchanged_last(u).wait_send()
    deliver_last(subs - 1)

    facing = lax.rem(i - j + nc, nc) == nc // 2
    with jax.named_scope("dxfinal"):
        for kk in range(2):
            own = (i == j) & (k == kk)

            @pl.when(own)
            def _():
                rest = dxb.at[pl.ds(0, kd - kq)]
                remote(rest, rest, s_dx.at[0], q_dx.at[kk], c=i, r=sib).wait_recv()

            @pl.when(facing)
            def _():
                rest = dxb.at[pl.ds(0, kd), pl.ds(0, runs * ROWS)]
                remote(rest, rest, s_dx.at[0], q_dx.at[kk], c=i, r=sib).wait_recv()
                rest = dxl.at[pl.ds(0, kd)]
                remote(rest, rest, s_dx.at[0], q_dxl.at[kk], c=i, r=sib).wait_recv()

            @pl.when(jnp.logical_not(own | facing))
            def _():
                rest = dxb.at[pl.ds(0, kd)]
                remote(rest, rest, s_dx.at[0], q_dx.at[kk], c=i, r=sib).wait_recv()

    with jax.named_scope("drain"):
        @pl.when(i != j)
        def _():
            away = st.at[pl.ds(0, nbig)]
            remote(away, away, s_dx.at[0], q_dx.at[0], c=i, r=sib).wait_send()

        away = st.at[pl.ds(0, early - nbig + runs + subs * 2 * 2 * SUB // m)]
        remote(away, away, s_dx.at[1], q_dx.at[0], c=i, r=sib).wait_send()


def _store(nc, dwv, dxb, dxl, dx, dw, dxo, sem):
    kd = dwv.shape[0]
    tb = dxb.shape[1]
    puts = []
    for p in range(PUTS):
        rows = pl.ds(p * (kd // PUTS), kd // PUTS)
        puts.append(pltpu.make_async_copy(dwv.at[rows], dw.at[rows], sem.at[p]))
    for put in puts:
        put.start()
    r = lax.axis_index("r")
    i, k = r // 2, lax.rem(r, 2)
    facing = lax.rem(i - lax.axis_index("c") + nc, nc) == nc // 2
    dxo[:tb - ROWS] = dxb[:, :tb - ROWS].T
    for kk in range(2):
        rows = pl.ds(kk * kd, kd)
        runs = [dxl[rows, u * 2 * SUB:(u + 1) * 2 * SUB] for u in range(ROWS // SUB)]
        a = jnp.concatenate([run[:, :SUB] for run in runs], axis=1)
        b = jnp.concatenate([run[:, SUB:] for run in runs], axis=1)
        late = jnp.where(facing, jnp.where(k == kk, a, b), dxb[rows, tb - ROWS:])
        dxo[tb - ROWS:, kk * kd:(kk + 1) * kd] = late.T
    puts.append(pltpu.make_async_copy(dxo, dx, sem.at[PUTS]))
    puts[-1].start()
    for put in puts:
        put.wait()


def solution(mesh):
    nr, nc = mesh.shape["r"], mesh.shape["c"]

    def local(x, w, dy):
        tb, kb = x.shape
        kd, nb = w.shape
        m = 2 * ROWS
        nbig, runs, subs = tb // m, tb // ROWS - 1, ROWS // SUB
        nsteps = 6 * nbig + runs
        kq = kd // nc
        bf16, f32 = jnp.bfloat16, jnp.float32
        dma = pltpu.SemaphoreType.DMA
        any_ = pl.BlockSpec(memory_space=pl.ANY)
        vmem = pl.BlockSpec(memory_space=pltpu.VMEM)
        outs = kd * nb * 4 + kb * (tb + 2 * ROWS) * 2
        dwv, dxb, dxl, _ = pl.pallas_call(
            functools.partial(_main, nr, nc),
            name="linear_backward",
            out_shape=(pltpu.VMEM((kd, nb), f32), pltpu.VMEM((kb, tb), bf16),
                       pltpu.VMEM((kb, 2 * ROWS), bf16), jax.ShapeDtypeStruct((nr, tb, nb), bf16)),
            in_specs=[any_] * 3,
            out_specs=(vmem, vmem, vmem, any_),
            scratch_shapes=[
                pltpu.VMEM((2, m, nb), bf16), pltpu.VMEM((m, nb), bf16), pltpu.VMEM((kd, nb), bf16),
                pltpu.VMEM((tb, kb), bf16), pltpu.VMEM((kb, tb), bf16), pltpu.VMEM((nc, 2, kd // nc, tb), bf16),
                pltpu.VMEM((nr, kd, tb), bf16), pltpu.VMEM((3, kd, m), f32), pltpu.VMEM((subs, kd, 2 * SUB), f32),
                pltpu.VMEM((nc - 1, nsteps, kq, m), f32), pltpu.VMEM((nc - 1, subs, kq, 2 * SUB), f32),
                pltpu.VMEM((nsteps, kq, m), bf16), pltpu.VMEM((subs, kq, 2 * SUB), bf16),
                dma((2,)), dma((2,)), dma((3,)), dma, dma((nbig,)), dma((nbig,)), dma((3, nbig)),
                dma((2, runs)), dma((runs,)), dma, dma((2, subs)), dma((subs,)),
                dma((3,)), dma((3,)), dma((3 + subs,)), dma((nsteps + subs,)), dma((2,)), dma((2,)), dma((2,)), dma((4,)),
            ],
            compiler_params=pltpu.CompilerParams(collective_id=0, has_side_effects=True,
                                                 vmem_limit_bytes=VMEM - outs - 2**21),
        )(x, w, dy)
        return pl.pallas_call(
            functools.partial(_store, nc),
            name="store",
            out_shape=(jax.ShapeDtypeStruct((tb, kb), bf16), jax.ShapeDtypeStruct((kd, nb), f32)),
            in_specs=[vmem] * 3,
            out_specs=(any_, any_),
            scratch_shapes=[pltpu.VMEM((tb, kb), bf16), dma((PUTS + 1,))],
            compiler_params=pltpu.CompilerParams(vmem_limit_bytes=2**22),
        )(dwv, dxb, dxl)

    act = P(("dp", "r"), "c")
    return jax.shard_map(local, mesh=mesh, in_specs=(act, P("r", "c"), act),
                         out_specs=(act, act), check_vma=False)
```

```python
import functools

import jax
import jax.numpy as jnp
from jax import lax
from jax.experimental import pallas as pl
from jax.experimental.pallas import tpu as pltpu
from jax.sharding import PartitionSpec as P

MESH = pl.DeviceIdType.MESH
ROWS = 128
FIRST = 3
MORE = 13
THEN = 15
SUB = 64
TILE = 1024
VMEM = 67043328
PUTS = 4


def _main(nr, nc, x, w, dy, dwv, dxb, dxl, dyg,
          dyb, dyl, wv, xin, xts, x0, xt, pb, pt, rb, rt, st, stl,
          s_own, s_fwd, s_sib, s_opp, q_left, q_right, q_sib, q_fwd, q_opp, s_last, q_last, q_slast,
          s_x, q_x, s_part, q_part, s_dx, q_dx, q_dxl, lsem):
    r = lax.axis_index("r")
    j = lax.axis_index("c")
    i, k = r // 2, lax.rem(r, 2)
    tb = x.shape[0]
    kd, nb = w.shape
    kq = kd // nc
    half = nb // 2
    m = 2 * ROWS
    nbig = tb // m
    early = 6 * nbig
    runs = tb // ROWS - 1
    steps = early + runs
    subs = ROWS // SUB

    def rot(d):
        return lax.rem(r + d + nr, nr)

    right, left, opp = rot(2), rot(-2), rot(nr // 2)
    sib = r + 1 - 2 * k
    sibright, sibleft, sibopp = lax.rem(sib + 2, nr), lax.rem(sib - 2 + nr, nr), lax.rem(sib + nr // 2, nr)

    def remote(src, dst, s, q, **dev):
        return pltpu.make_async_remote_copy(src_ref=src, dst_ref=dst, send_sem=s, recv_sem=q,
                                            device_id=dev, device_id_type=MESH)

    def at(start, size):
        return pl.ds(pl.multiple_of(start, size), size)

    load_x = pltpu.make_async_copy(x, xin, lsem.at[0])
    load_w = pltpu.make_async_copy(w, wv, lsem.at[1])
    load_x.start()
    load_w.start()
    bar = pltpu.get_barrier_semaphore()
    for dc in range(nc):
        for dr in range(nr):
            if dc or dr:
                pl.semaphore_signal(bar, inc=1, device_id={"c": lax.rem(j + dc, nc), "r": lax.rem(r + dr, nr)},
                                    device_id_type=MESH)
    pl.semaphore_wait(bar, nc * nr - 1)

    def own_right(row, size):
        rows = pl.ds(row, size)
        return remote(dy.at[rows], dyg.at[r, rows], s_own.at[0], q_left.at[row // m], r=right)

    def own_left(row, size):
        rows = pl.ds(row, size)
        return remote(dy.at[rows], dyg.at[r, rows], s_own.at[1], q_right.at[row // m], r=left)

    def to_sib(blk, kind, c):
        src = dy.at[at(c * m, m)] if kind == 0 else dyg.at[blk, at(c * m, m)]
        return remote(src, dyg.at[blk, at(c * m, m)], s_sib.at[kind], q_sib.at[kind, c], r=sib)

    def wait_left(c):
        remote(dy.at[at(c * m, m)], dyg.at[left, at(c * m, m)], s_own.at[0], q_left.at[c], r=right).wait_recv()

    def wait_right(c):
        remote(dy.at[at(c * m, m)], dyg.at[right, at(c * m, m)], s_own.at[1], q_right.at[c], r=left).wait_recv()

    def part(blk, h, row, size):
        return dyg.at[blk, at(row, size), pl.ds(h * half, half)]

    def forward(h, row, size, q):
        blk, to = ((left, right), (right, left))[h]
        return remote(part(blk, h, row, size), part(blk, h, row, size), s_fwd.at[h], q_fwd.at[h, q], r=to)

    def opp_in(h, row, size, q):
        return remote(part(opp, h, row, size), part(opp, h, row, size), s_fwd.at[h], q_fwd.at[h, q], r=right)

    def opp_sib(h, row, size, q):
        return remote(part(opp, h, row, size), part(opp, h, row, size), s_opp, q_opp.at[q], r=sib)

    def wait_opp_sib(row, size, q):
        rows = dyg.at[sibopp, at(row, size)]
        remote(rows, rows, s_opp, q_opp.at[q], r=sib).wait_recv()

    def last(h, u, row):
        return dyl.at[pl.ds(pl.multiple_of(row + u * SUB, SUB), SUB), pl.ds(h * half, half)]

    def forward_last(h, u):
        blk, to = ((left, right), (right, left))[h]
        return remote(part(blk, h, tb - ROWS + u * SUB, SUB), last(h, u, 0), s_fwd.at[h], q_last.at[h, u], r=to)

    def sib_last(h, u):
        return remote(last(h, u, 0), last(h, u, ROWS), s_last, q_slast.at[u], r=sib)

    own_right(0, ROWS).start()
    own_left(0, ROWS).start()

    load_x.wait()
    xts[...] = xin[...].T
    for kk in range(2):
        x0[j, kk] = xts[pl.ds(pl.multiple_of(kk * kd + j * kq, 16), kq)]
    mine = pl.ds(pl.multiple_of(j * kq, 16), kq)

    for dq in range(1, nc):
        for kk in range(2):
            q = lax.rem(j + dq, nc)
            remote(xts.at[pl.ds(pl.multiple_of(kk * kd + q * kq, 16), kq)], x0.at[j, kk],
                   s_x.at[0], q_x.at[0], c=q).start()
    spread = remote(x0.at[pl.ds(0, nc - 1)], x0.at[pl.ds(0, nc - 1)], s_x.at[0], q_x.at[0], c=lax.rem(j + 1, nc))

    def zero(t, _):
        dwv[:, at(t * TILE, TILE)] = jnp.zeros((kd, TILE), jnp.float32)
        return 0

    lax.fori_loop(0, nb // TILE, zero, 0)
    with jax.named_scope("xspread"):
        spread.wait_recv()
    for d in range(1, nr):
        t = lax.rem(r + d, nr)
        remote(x0.at[t // 2, lax.rem(t, 2)], xt.at[r, mine], s_x.at[1], q_x.at[1], r=t).start()
    cross = remote(xt.at[pl.ds(0, nr - 1), mine], xt.at[pl.ds(0, nr - 1), mine], s_x.at[1], q_x.at[1], r=right)
    xt[r, mine] = x0[i, k]
    own_right(ROWS, ROWS).start()
    own_left(ROWS, ROWS).start()
    to_sib(r, 0, 0).start()
    for c in range(1, nbig):
        own_right(c * m, m).start()
        own_left(c * m, m).start()
        to_sib(r, 0, c).start()
    with jax.named_scope("xcross"):
        cross.wait_recv()
    for dq in range(1, nc):
        remote(xt.at[:, mine], xt.at[:, mine], s_x.at[2], q_x.at[2], c=lax.rem(j + dq, nc)).start()
    others = pl.ds(0, (nc - 1) * kq)
    gather = remote(xt.at[:, others], xt.at[:, others], s_x.at[2], q_x.at[2], c=lax.rem(j + 1, nc))
    load_w.wait()

    def where(s):
        t = s - 2 * nbig
        kind = lax.rem(t, 4)
        late = s >= early
        blk = jnp.where(s < nbig, r, jnp.where(s < 2 * nbig, sib, jnp.where(
            kind == 0, left, jnp.where(kind == 1, right, jnp.where(kind == 2, sibleft, sibright)))))
        c = 2 * jnp.where(s < 2 * nbig, lax.rem(s, nbig), t // 4)
        blka = jnp.where(late, opp, blk)
        blkb = jnp.where(late, sibopp, blk)
        ca = jnp.where(late, s - early, c)
        cb = jnp.where(late, s - early, c + 1)
        return blka, ca, blkb, cb

    def fetch(src, blk, row, size, slot, to, h):
        rows = src.at[at(row, size)] if blk is None else src.at[blk, at(row, size)]
        return pltpu.make_async_copy(rows, dyb.at[slot, pl.ds(to, size)], lsem.at[2 + h])

    def arrive(s):
        blka, ca, blkb, cb = where(s)
        slot = lax.rem(s, 2)
        t = s - 2 * nbig
        kind = lax.rem(t, 4)
        c = t // 4
        mid = (s >= 2 * nbig) & (s < early)

        @pl.when((s >= nbig) & (s < 2 * nbig))
        def _():
            to_sib(sib, 0, s - nbig).wait_recv()

        for h in range(2):
            @pl.when(mid & (kind == h))
            def _():
                (wait_left, wait_right)[h](c)

                forward(h, 2 * c * ROWS, ROWS, 2 * c).start()

                @pl.when(c < nbig - 1)
                def _():
                    forward(h, (2 * c + 1) * ROWS, ROWS, 2 * c + 1).start()

                @pl.when(c == nbig - 1)
                def _():
                    for u in range(subs):
                        forward_last(h, u).start()

                to_sib((left, right)[h], 1 + h, c).start()

            @pl.when(mid & (kind == 2 + h))
            def _():
                to_sib((sibleft, sibright)[h], 1 + h, c).wait_recv()

        @pl.when(s < nbig)
        def _():
            fetch(dy, None, ca * ROWS, ROWS, slot, 0, 0).start()
            fetch(dy, None, cb * ROWS, ROWS, slot, ROWS, 1).start()

        @pl.when(s >= nbig)
        def _():
            @pl.when(s >= early)
            def _():
                with jax.named_scope("opp"):
                    for h in range(2):
                        opp_in(h, ca * ROWS, ROWS, ca).wait_recv()
                        opp_sib(h, ca * ROWS, ROWS, ca).start()

            fetch(dyg, blka, ca * ROWS, ROWS, slot, 0, 0).start()

            @pl.when(s >= early)
            def _():
                with jax.named_scope("oppsib"):
                    wait_opp_sib(ca * ROWS, ROWS, ca)

            fetch(dyg, blkb, cb * ROWS, ROWS, slot, ROWS, 1).start()

    def exchange(s):
        ps = lax.rem(s, 3)
        for dq in range(1, nc):
            q = lax.rem(j + dq, nc)
            remote(pb.at[ps, pl.ds(pl.multiple_of(q * kq, 16), kq)], rb.at[dq - 1, s], s_part.at[ps], q_part.at[s], c=q).start()

    def exchanged(s):
        ps = lax.rem(s, 3)
        rows = pl.ds(0, (nc - 1) * kq)
        return remote(pb.at[ps, rows], pb.at[ps, rows], s_part.at[ps], q_part.at[s], c=lax.rem(j + 1, nc))

    def sum_step(s):
        exchanged(s).wait_recv()
        acc = pb[lax.rem(s, 3), mine]
        for dq in range(1, nc):
            acc += rb[dq - 1, s]
        st[s] = acc.astype(jnp.bfloat16)

    def send_dx(s, lanes, blk, row, size):
        src = st.at[s, :, lanes]
        share = pl.ds(pl.multiple_of(k * kd + j * kq, 16), kq)
        dst = dxb.at[share, at(row, size)]

        @pl.when(blk != r)
        def _():
            remote(src, dst, s_dx.at[1], q_dx.at[k], c=i, r=blk).start()

        @pl.when((blk == r) & (i != j))
        def _():
            remote(src, dst, s_dx.at[0], q_dx.at[k], c=i, r=blk).start()

        @pl.when((blk == r) & (i == j))
        def _():
            dxb[share, at(row, size)] = st[s, :, lanes]

    def deliver_early(s):
        blka, ca, _, _ = where(s)
        for h in range(2):
            send_dx(s, pl.ds(h * ROWS, ROWS), blka, (ca + h) * ROWS, ROWS)

    def deliver_late(s):
        blka, ca, blkb, cb = where(s)
        send_dx(s, pl.ds(0, ROWS), blka, ca * ROWS, ROWS)
        send_dx(s, pl.ds(ROWS, ROWS), blkb, cb * ROWS, ROWS)

    def exchange_last(u):
        for dq in range(1, nc):
            q = lax.rem(j + dq, nc)
            remote(pt.at[u, pl.ds(pl.multiple_of(q * kq, 16), kq)], rt.at[dq - 1, u], s_part.at[3 + u], q_part.at[steps + u],
                   c=q).start()

    def exchanged_last(u):
        rows = pl.ds(0, (nc - 1) * kq)
        return remote(pt.at[u, rows], pt.at[u, rows], s_part.at[3 + u], q_part.at[steps + u], c=lax.rem(j + 1, nc))

    def sum_last(u):
        exchanged_last(u).wait_recv()
        acc = pt[u, mine]
        for dq in range(1, nc):
            acc += rt[dq - 1, u]
        stl[u] = acc.astype(jnp.bfloat16)

    def deliver_last(u):
        share = pl.ds(pl.multiple_of(k * kd + j * kq, 16), kq)
        for blk in (opp, sibopp):
            remote(stl.at[u], dxl.at[share, at(u * 2 * SUB, 2 * SUB)], s_dx.at[1], q_dxl.at[k], c=i, r=blk).start()

    arrive(jnp.int32(0))
    with jax.named_scope("xgather"):
        gather.wait_recv()

    def dw_tiles(buf, blka, ca, blkb, cb, lo, hi):
        def dw_tile(t, _):
            cols = at(t * TILE, TILE)
            lhs = jnp.concatenate([xt[blka, :, at(ca * ROWS, ROWS)], xt[blkb, :, at(cb * ROWS, ROWS)]], axis=1)
            dwv[:, cols] += jnp.dot(lhs, buf[:, cols], preferred_element_type=jnp.float32)
            return 0

        lax.fori_loop(lo, hi, dw_tile, 0)

    def step(s, _):
        slot, ps = lax.rem(s, 2), lax.rem(s, 3)
        blka, ca, blkb, cb = where(s)

        @pl.when(s >= 3)
        def _():
            exchanged(s - 3).wait_send()

        with jax.named_scope("reduce"):
            @pl.when((s >= 2) & (s <= early))
            def _():
                sum_step(s - 2)

            @pl.when(s >= early)
            def _():
                sum_step(s - 1)

        with jax.named_scope("loadwait"):
            for h in range(2):
                fetch(dyg, r, 0, ROWS, slot, h * ROWS, h).wait()
        pb[ps] = jnp.zeros((kd, m), jnp.float32)

        def dx_tile(t, _):
            cols = at(t * TILE, TILE)
            pb[ps] += lax.dot_general(wv[:, cols], dyb[slot, :, cols], (((1,), (1,)), ((), ())),
                                      preferred_element_type=jnp.float32)
            return 0

        with jax.named_scope("dx"):
            lax.fori_loop(0, nb // TILE, dx_tile, 0)

        dw_tiles(dyb.at[slot], blka, ca, blkb, cb, 0, 1)
        exchange(s)

        @pl.when((s >= 2) & (s < FIRST + 2))
        def _():
            deliver_early(s - 2)

        per = -(-(MORE - FIRST) // runs)
        for d in range(per):
            old = FIRST + (s - early) * per + d

            @pl.when((s >= early) & (old < MORE))
            def _():
                deliver_early(old)

        @pl.when(s > early)
        def _():
            deliver_late(s - 1)

        @pl.when(s < early - 1)
        def _():
            arrive(s + 1)

        with jax.named_scope("dw"):
            dw_tiles(dyb.at[slot], blka, ca, blkb, cb, 1, nb // TILE)

        @pl.when((s >= early - 1) & (s < steps - 1))
        def _():
            arrive(s + 1)

        return 0

    lax.fori_loop(0, steps, step, 0)

    for u in range(subs):
        with jax.named_scope("opp"):
            for h in range(2):
                forward_last(h, u).wait_recv()
                sib_last(h, u).start()
        if u == 0:
            pt[...] = jnp.zeros((subs, kd, 2 * SUB), jnp.float32)
        with jax.named_scope("oppsib"):
            both = dyl.at[pl.ds(0, SUB)]
            remote(both, both, s_last, q_slast.at[u], r=sib).wait_recv()

        def dx_tile(t, _):
            cols = at(t * TILE, TILE)
            rhs = jnp.concatenate([dyl[pl.ds(u * SUB, SUB), cols], dyl[pl.ds(ROWS + u * SUB, SUB), cols]], axis=0)
            pt[u] += lax.dot_general(wv[:, cols], rhs, (((1,), (1,)), ((), ())), preferred_element_type=jnp.float32)
            return 0

        with jax.named_scope("dx"):
            lax.fori_loop(0, nb // TILE, dx_tile, 0)
        if u == subs - 1:
            dw_tiles(dyl, opp, runs, sibopp, runs, 0, 1)
        exchange_last(u)
        if u == 0:
            for old in range(MORE, THEN):
                deliver_early(jnp.int32(old))
            with jax.named_scope("reduce"):
                sum_step(steps - 1)

    deliver_late(steps - 1)
    for old in range(THEN, early):
        deliver_early(jnp.int32(old))
    with jax.named_scope("dw"):
        dw_tiles(dyl, opp, runs, sibopp, runs, 1, nb // TILE)
    for u in range(subs - 1):
        with jax.named_scope("reduce"):
            sum_last(u)
        deliver_last(u)

    for d in range(2):
        remote(dy, dyg.at[r], s_own.at[d], q_left.at[0], r=right).wait_send()
        remote(dyg.at[r, :, pl.ds(0, half)], dyg.at[r, :, pl.ds(0, half)], s_fwd.at[d], q_left.at[0], r=right).wait_send()
    for kind in range(3):
        remote(dy, dyg.at[r], s_sib.at[kind], q_left.at[0], r=right).wait_send()
    sent = dyg.at[r, pl.ds(0, runs * ROWS)]
    remote(sent, sent, s_opp, q_left.at[0], r=right).wait_send()
    sent = dyl.at[pl.ds(0, ROWS)]
    remote(sent, sent, s_last, q_left.at[0], r=right).wait_send()
    for sent in (spread, cross, gather):
        sent.wait_send()
    for s in range(steps - 3, steps):
        exchanged(s).wait_send()
    with jax.named_scope("reduce"):
        sum_last(subs - 1)
    for u in range(subs):
        exchanged_last(u).wait_send()
    deliver_last(subs - 1)

    facing = lax.rem(i - j + nc, nc) == nc // 2
    with jax.named_scope("dxfinal"):
        for kk in range(2):
            own = (i == j) & (k == kk)

            @pl.when(own)
            def _():
                rest = dxb.at[pl.ds(0, kd - kq)]
                remote(rest, rest, s_dx.at[0], q_dx.at[kk], c=i, r=sib).wait_recv()

            @pl.when(facing)
            def _():
                rest = dxb.at[pl.ds(0, kd), pl.ds(0, runs * ROWS)]
                remote(rest, rest, s_dx.at[0], q_dx.at[kk], c=i, r=sib).wait_recv()
                rest = dxl.at[pl.ds(0, kd)]
                remote(rest, rest, s_dx.at[0], q_dxl.at[kk], c=i, r=sib).wait_recv()

            @pl.when(jnp.logical_not(own | facing))
            def _():
                rest = dxb.at[pl.ds(0, kd)]
                remote(rest, rest, s_dx.at[0], q_dx.at[kk], c=i, r=sib).wait_recv()

    with jax.named_scope("drain"):
        @pl.when(i != j)
        def _():
            away = st.at[pl.ds(0, nbig)]
            remote(away, away, s_dx.at[0], q_dx.at[0], c=i, r=sib).wait_send()

        away = st.at[pl.ds(0, early - nbig + runs + subs * 2 * 2 * SUB // m)]
        remote(away, away, s_dx.at[1], q_dx.at[0], c=i, r=sib).wait_send()


def _store(nc, dwv, dxb, dxl, dx, dw, dxo, sem):
    kd = dwv.shape[0]
    tb = dxb.shape[1]
    puts = []
    for p in range(PUTS):
        rows = pl.ds(p * (kd // PUTS), kd // PUTS)
        puts.append(pltpu.make_async_copy(dwv.at[rows], dw.at[rows], sem.at[p]))
    for put in puts:
        put.start()
    r = lax.axis_index("r")
    i, k = r // 2, lax.rem(r, 2)
    facing = lax.rem(i - lax.axis_index("c") + nc, nc) == nc // 2
    dxo[:tb - ROWS] = dxb[:, :tb - ROWS].T
    for kk in range(2):
        rows = pl.ds(kk * kd, kd)
        runs = [dxl[rows, u * 2 * SUB:(u + 1) * 2 * SUB] for u in range(ROWS // SUB)]
        a = jnp.concatenate([run[:, :SUB] for run in runs], axis=1)
        b = jnp.concatenate([run[:, SUB:] for run in runs], axis=1)
        late = jnp.where(facing, jnp.where(k == kk, a, b), dxb[rows, tb - ROWS:])
        dxo[tb - ROWS:, kk * kd:(kk + 1) * kd] = late.T
    puts.append(pltpu.make_async_copy(dxo, dx, sem.at[PUTS]))
    puts[-1].start()
    for put in puts:
        put.wait()


def solution(mesh):
    nr, nc = mesh.shape["r"], mesh.shape["c"]

    def local(x, w, dy):
        tb, kb = x.shape
        kd, nb = w.shape
        m = 2 * ROWS
        nbig, runs, subs = tb // m, tb // ROWS - 1, ROWS // SUB
        nsteps = 6 * nbig + runs
        kq = kd // nc
        bf16, f32 = jnp.bfloat16, jnp.float32
        dma = pltpu.SemaphoreType.DMA
        any_ = pl.BlockSpec(memory_space=pl.ANY)
        vmem = pl.BlockSpec(memory_space=pltpu.VMEM)
        outs = kd * nb * 4 + kb * (tb + 2 * ROWS) * 2
        dwv, dxb, dxl, _ = pl.pallas_call(
            functools.partial(_main, nr, nc),
            name="linear_backward",
            out_shape=(pltpu.VMEM((kd, nb), f32), pltpu.VMEM((kb, tb), bf16),
                       pltpu.VMEM((kb, 2 * ROWS), bf16), jax.ShapeDtypeStruct((nr, tb, nb), bf16)),
            in_specs=[any_] * 3,
            out_specs=(vmem, vmem, vmem, any_),
            scratch_shapes=[
                pltpu.VMEM((2, m, nb), bf16), pltpu.VMEM((m, nb), bf16), pltpu.VMEM((kd, nb), bf16),
                pltpu.VMEM((tb, kb), bf16), pltpu.VMEM((kb, tb), bf16), pltpu.VMEM((nc, 2, kd // nc, tb), bf16),
                pltpu.VMEM((nr, kd, tb), bf16), pltpu.VMEM((3, kd, m), f32), pltpu.VMEM((subs, kd, 2 * SUB), f32),
                pltpu.VMEM((nc - 1, nsteps, kq, m), f32), pltpu.VMEM((nc - 1, subs, kq, 2 * SUB), f32),
                pltpu.VMEM((nsteps, kq, m), bf16), pltpu.VMEM((subs, kq, 2 * SUB), bf16),
                dma((2,)), dma((2,)), dma((3,)), dma, dma((nbig,)), dma((nbig,)), dma((3, nbig)),
                dma((2, runs)), dma((runs,)), dma, dma((2, subs)), dma((subs,)),
                dma((3,)), dma((3,)), dma((3 + subs,)), dma((nsteps + subs,)), dma((2,)), dma((2,)), dma((2,)), dma((4,)),
            ],
            compiler_params=pltpu.CompilerParams(collective_id=0, has_side_effects=True,
                                                 vmem_limit_bytes=VMEM - outs - 2**21),
        )(x, w, dy)
        return pl.pallas_call(
            functools.partial(_store, nc),
            name="store",
            out_shape=(jax.ShapeDtypeStruct((tb, kb), bf16), jax.ShapeDtypeStruct((kd, nb), f32)),
            in_specs=[vmem] * 3,
            out_specs=(any_, any_),
            scratch_shapes=[pltpu.VMEM((tb, kb), bf16), dma((PUTS + 1,))],
            compiler_params=pltpu.CompilerParams(vmem_limit_bytes=2**22),
        )(dwv, dxb, dxl)

    act = P(("dp", "r"), "c")
    return jax.shard_map(local, mesh=mesh, in_specs=(act, P("r", "c"), act),
                         out_specs=(act, act), check_vma=False)
```

```python
import functools

import jax
import jax.numpy as jnp
from jax import lax
from jax.experimental import pallas as pl
from jax.experimental.pallas import tpu as pltpu
from jax.sharding import PartitionSpec as P

MESH = pl.DeviceIdType.MESH
ROWS = 128
FIRST = 3
MORE = 13
THEN = 15
SUB = 64
TILE = 1024
VMEM = 67043328
PUTS = 4


def _main(nr, nc, x, w, dy, dwv, dxb, dxl, dyg,
          dyb, dyl, wv, xin, xts, x0, xt, pb, pt, rb, rt, st, stl,
          s_own, s_fwd, s_sib, s_opp, q_left, q_right, q_sib, q_fwd, q_opp, s_last, q_last, q_slast,
          s_x, q_x, s_part, q_part, s_dx, q_dx, q_dxl, lsem):
    r = lax.axis_index("r")
    j = lax.axis_index("c")
    i, k = r // 2, lax.rem(r, 2)
    tb = x.shape[0]
    kd, nb = w.shape
    kq = kd // nc
    half = nb // 2
    m = 2 * ROWS
    nbig = tb // m
    early = 6 * nbig
    runs = tb // ROWS - 1
    steps = early + runs
    subs = ROWS // SUB

    def rot(d):
        return lax.rem(r + d + nr, nr)

    right, left, opp = rot(2), rot(-2), rot(nr // 2)
    sib = r + 1 - 2 * k
    sibright, sibleft, sibopp = lax.rem(sib + 2, nr), lax.rem(sib - 2 + nr, nr), lax.rem(sib + nr // 2, nr)

    def remote(src, dst, s, q, **dev):
        return pltpu.make_async_remote_copy(src_ref=src, dst_ref=dst, send_sem=s, recv_sem=q,
                                            device_id=dev, device_id_type=MESH)

    def at(start, size):
        return pl.ds(pl.multiple_of(start, size), size)

    load_x = pltpu.make_async_copy(x, xin, lsem.at[0])
    load_w = pltpu.make_async_copy(w, wv, lsem.at[1])
    load_x.start()
    load_w.start()
    bar = pltpu.get_barrier_semaphore()
    for dc in range(nc):
        for dr in range(nr):
            if dc or dr:
                pl.semaphore_signal(bar, inc=1, device_id={"c": lax.rem(j + dc, nc), "r": lax.rem(r + dr, nr)},
                                    device_id_type=MESH)
    pl.semaphore_wait(bar, nc * nr - 1)

    def own_right(row, size):
        rows = pl.ds(row, size)
        return remote(dy.at[rows], dyg.at[r, rows], s_own.at[0], q_left.at[row // m], r=right)

    def own_left(row, size):
        rows = pl.ds(row, size)
        return remote(dy.at[rows], dyg.at[r, rows], s_own.at[1], q_right.at[row // m], r=left)

    def to_sib(blk, kind, c):
        src = dy.at[at(c * m, m)] if kind == 0 else dyg.at[blk, at(c * m, m)]
        return remote(src, dyg.at[blk, at(c * m, m)], s_sib.at[kind], q_sib.at[kind, c], r=sib)

    def wait_left(c):
        remote(dy.at[at(c * m, m)], dyg.at[left, at(c * m, m)], s_own.at[0], q_left.at[c], r=right).wait_recv()

    def wait_right(c):
        remote(dy.at[at(c * m, m)], dyg.at[right, at(c * m, m)], s_own.at[1], q_right.at[c], r=left).wait_recv()

    def part(blk, h, row, size):
        return dyg.at[blk, at(row, size), pl.ds(h * half, half)]

    def forward(h, row, size, q):
        blk, to = ((left, right), (right, left))[h]
        return remote(part(blk, h, row, size), part(blk, h, row, size), s_fwd.at[h], q_fwd.at[h, q], r=to)

    def opp_in(h, row, size, q):
        return remote(part(opp, h, row, size), part(opp, h, row, size), s_fwd.at[h], q_fwd.at[h, q], r=right)

    def opp_sib(h, row, size, q):
        return remote(part(opp, h, row, size), part(opp, h, row, size), s_opp, q_opp.at[q], r=sib)

    def wait_opp_sib(row, size, q):
        rows = dyg.at[sibopp, at(row, size)]
        remote(rows, rows, s_opp, q_opp.at[q], r=sib).wait_recv()

    def last(h, u, row):
        return dyl.at[pl.ds(pl.multiple_of(row + u * SUB, SUB), SUB), pl.ds(h * half, half)]

    def forward_last(h, u):
        blk, to = ((left, right), (right, left))[h]
        return remote(part(blk, h, tb - ROWS + u * SUB, SUB), last(h, u, 0), s_fwd.at[h], q_last.at[h, u], r=to)

    def sib_last(h, u):
        return remote(last(h, u, 0), last(h, u, ROWS), s_last, q_slast.at[u], r=sib)

    own_right(0, ROWS).start()
    own_left(0, ROWS).start()

    load_x.wait()
    xts[...] = xin[...].T
    for kk in range(2):
        x0[j, kk] = xts[pl.ds(pl.multiple_of(kk * kd + j * kq, 16), kq)]
    mine = pl.ds(pl.multiple_of(j * kq, 16), kq)

    for dq in range(1, nc):
        for kk in range(2):
            q = lax.rem(j + dq, nc)
            remote(xts.at[pl.ds(pl.multiple_of(kk * kd + q * kq, 16), kq)], x0.at[j, kk],
                   s_x.at[0], q_x.at[0], c=q).start()
    spread = remote(x0.at[pl.ds(0, nc - 1)], x0.at[pl.ds(0, nc - 1)], s_x.at[0], q_x.at[0], c=lax.rem(j + 1, nc))

    def zero(t, _):
        dwv[:, at(t * TILE, TILE)] = jnp.zeros((kd, TILE), jnp.float32)
        return 0

    lax.fori_loop(0, nb // TILE, zero, 0)
    with jax.named_scope("xspread"):
        spread.wait_recv()
    for d in range(1, nr):
        t = lax.rem(r + d, nr)
        remote(x0.at[t // 2, lax.rem(t, 2)], xt.at[r, mine], s_x.at[1], q_x.at[1], r=t).start()
    cross = remote(xt.at[pl.ds(0, nr - 1), mine], xt.at[pl.ds(0, nr - 1), mine], s_x.at[1], q_x.at[1], r=right)
    xt[r, mine] = x0[i, k]
    own_right(ROWS, ROWS).start()
    own_left(ROWS, ROWS).start()
    to_sib(r, 0, 0).start()
    for c in range(1, nbig):
        own_right(c * m, m).start()
        own_left(c * m, m).start()
        to_sib(r, 0, c).start()
    with jax.named_scope("xcross"):
        cross.wait_recv()
    for dq in range(1, nc):
        remote(xt.at[:, mine], xt.at[:, mine], s_x.at[2], q_x.at[2], c=lax.rem(j + dq, nc)).start()
    others = pl.ds(0, (nc - 1) * kq)
    gather = remote(xt.at[:, others], xt.at[:, others], s_x.at[2], q_x.at[2], c=lax.rem(j + 1, nc))
    load_w.wait()

    def where(s):
        t = s - 2 * nbig
        kind = lax.rem(t, 4)
        late = s >= early
        blk = jnp.where(s < nbig, r, jnp.where(s < 2 * nbig, sib, jnp.where(
            kind == 0, left, jnp.where(kind == 1, right, jnp.where(kind == 2, sibleft, sibright)))))
        c = 2 * jnp.where(s < 2 * nbig, lax.rem(s, nbig), t // 4)
        blka = jnp.where(late, opp, blk)
        blkb = jnp.where(late, sibopp, blk)
        ca = jnp.where(late, s - early, c)
        cb = jnp.where(late, s - early, c + 1)
        return blka, ca, blkb, cb

    def fetch(src, blk, row, size, slot, to, h):
        rows = src.at[at(row, size)] if blk is None else src.at[blk, at(row, size)]
        return pltpu.make_async_copy(rows, dyb.at[slot, pl.ds(to, size)], lsem.at[2 + h])

    def arrive(s):
        blka, ca, blkb, cb = where(s)
        slot = lax.rem(s, 2)
        t = s - 2 * nbig
        kind = lax.rem(t, 4)
        c = t // 4
        mid = (s >= 2 * nbig) & (s < early)

        @pl.when((s >= nbig) & (s < 2 * nbig))
        def _():
            to_sib(sib, 0, s - nbig).wait_recv()

        for h in range(2):
            @pl.when(mid & (kind == h))
            def _():
                (wait_left, wait_right)[h](c)

                forward(h, 2 * c * ROWS, ROWS, 2 * c).start()

                @pl.when(c < nbig - 1)
                def _():
                    forward(h, (2 * c + 1) * ROWS, ROWS, 2 * c + 1).start()

                @pl.when(c == nbig - 1)
                def _():
                    for u in range(subs):
                        forward_last(h, u).start()

                to_sib((left, right)[h], 1 + h, c).start()

            @pl.when(mid & (kind == 2 + h))
            def _():
                to_sib((sibleft, sibright)[h], 1 + h, c).wait_recv()

        @pl.when(s < nbig)
        def _():
            fetch(dy, None, ca * ROWS, ROWS, slot, 0, 0).start()
            fetch(dy, None, cb * ROWS, ROWS, slot, ROWS, 1).start()

        @pl.when(s >= nbig)
        def _():
            @pl.when(s >= early)
            def _():
                with jax.named_scope("opp"):
                    for h in range(2):
                        opp_in(h, ca * ROWS, ROWS, ca).wait_recv()
                        opp_sib(h, ca * ROWS, ROWS, ca).start()

            fetch(dyg, blka, ca * ROWS, ROWS, slot, 0, 0).start()

            @pl.when(s >= early)
            def _():
                with jax.named_scope("oppsib"):
                    wait_opp_sib(ca * ROWS, ROWS, ca)

            fetch(dyg, blkb, cb * ROWS, ROWS, slot, ROWS, 1).start()

    def exchange(s):
        ps = lax.rem(s, 3)
        for dq in range(1, nc):
            q = lax.rem(j + dq, nc)
            remote(pb.at[ps, pl.ds(pl.multiple_of(q * kq, 16), kq)], rb.at[dq - 1, s], s_part.at[ps], q_part.at[s], c=q).start()

    def exchanged(s):
        ps = lax.rem(s, 3)
        rows = pl.ds(0, (nc - 1) * kq)
        return remote(pb.at[ps, rows], pb.at[ps, rows], s_part.at[ps], q_part.at[s], c=lax.rem(j + 1, nc))

    def sum_step(s):
        exchanged(s).wait_recv()
        acc = pb[lax.rem(s, 3), mine]
        for dq in range(1, nc):
            acc += rb[dq - 1, s]
        st[s] = acc.astype(jnp.bfloat16)

    def send_dx(s, lanes, blk, row, size):
        src = st.at[s, :, lanes]
        share = pl.ds(pl.multiple_of(k * kd + j * kq, 16), kq)
        dst = dxb.at[share, at(row, size)]

        @pl.when(blk != r)
        def _():
            remote(src, dst, s_dx.at[1], q_dx.at[k], c=i, r=blk).start()

        @pl.when((blk == r) & (i != j))
        def _():
            remote(src, dst, s_dx.at[0], q_dx.at[k], c=i, r=blk).start()

        @pl.when((blk == r) & (i == j))
        def _():
            dxb[share, at(row, size)] = st[s, :, lanes]

    def deliver_early(s):
        blka, ca, _, _ = where(s)
        for h in range(2):
            send_dx(s, pl.ds(h * ROWS, ROWS), blka, (ca + h) * ROWS, ROWS)

    def deliver_late(s):
        blka, ca, blkb, cb = where(s)
        send_dx(s, pl.ds(0, ROWS), blka, ca * ROWS, ROWS)
        send_dx(s, pl.ds(ROWS, ROWS), blkb, cb * ROWS, ROWS)

    def exchange_last(u):
        for dq in range(1, nc):
            q = lax.rem(j + dq, nc)
            remote(pt.at[u, pl.ds(pl.multiple_of(q * kq, 16), kq)], rt.at[dq - 1, u], s_part.at[3 + u], q_part.at[steps + u],
                   c=q).start()

    def exchanged_last(u):
        rows = pl.ds(0, (nc - 1) * kq)
        return remote(pt.at[u, rows], pt.at[u, rows], s_part.at[3 + u], q_part.at[steps + u], c=lax.rem(j + 1, nc))

    def sum_last(u):
        exchanged_last(u).wait_recv()
        acc = pt[u, mine]
        for dq in range(1, nc):
            acc += rt[dq - 1, u]
        stl[u] = acc.astype(jnp.bfloat16)

    def deliver_last(u):
        share = pl.ds(pl.multiple_of(k * kd + j * kq, 16), kq)
        for blk in (opp, sibopp):
            remote(stl.at[u], dxl.at[share, at(u * 2 * SUB, 2 * SUB)], s_dx.at[1], q_dxl.at[k], c=i, r=blk).start()

    arrive(jnp.int32(0))
    with jax.named_scope("xgather"):
        gather.wait_recv()

    def dw_tiles(buf, blka, ca, blkb, cb, lo, hi):
        def dw_tile(t, _):
            cols = at(t * TILE, TILE)
            lhs = jnp.concatenate([xt[blka, :, at(ca * ROWS, ROWS)], xt[blkb, :, at(cb * ROWS, ROWS)]], axis=1)
            dwv[:, cols] += jnp.dot(lhs, buf[:, cols], preferred_element_type=jnp.float32)
            return 0

        lax.fori_loop(lo, hi, dw_tile, 0)

    def step(s, _):
        slot, ps = lax.rem(s, 2), lax.rem(s, 3)
        blka, ca, blkb, cb = where(s)

        @pl.when(s >= 3)
        def _():
            exchanged(s - 3).wait_send()

        with jax.named_scope("reduce"):
            @pl.when((s >= 2) & (s <= early))
            def _():
                sum_step(s - 2)

            @pl.when(s >= early)
            def _():
                sum_step(s - 1)

        with jax.named_scope("loadwait"):
            for h in range(2):
                fetch(dyg, r, 0, ROWS, slot, h * ROWS, h).wait()
        pb[ps] = jnp.zeros((kd, m), jnp.float32)

        def dx_tile(t, _):
            cols = at(t * TILE, TILE)
            pb[ps] += lax.dot_general(wv[:, cols], dyb[slot, :, cols], (((1,), (1,)), ((), ())),
                                      preferred_element_type=jnp.float32)
            return 0

        with jax.named_scope("dx"):
            lax.fori_loop(0, nb // TILE, dx_tile, 0)

        dw_tiles(dyb.at[slot], blka, ca, blkb, cb, 0, 1)
        exchange(s)

        @pl.when((s >= 2) & (s < FIRST + 2))
        def _():
            deliver_early(s - 2)

        @pl.when(s > early)
        def _():
            deliver_late(s - 1)

        per = -(-(MORE - FIRST) // runs)
        for d in range(per):
            old = FIRST + (s - early) * per + d

            @pl.when((s >= early) & (old < MORE))
            def _():
                deliver_early(old)

        @pl.when(s < early - 1)
        def _():
            arrive(s + 1)

        with jax.named_scope("dw"):
            dw_tiles(dyb.at[slot], blka, ca, blkb, cb, 1, nb // TILE)

        @pl.when((s >= early - 1) & (s < steps - 1))
        def _():
            arrive(s + 1)

        return 0

    lax.fori_loop(0, steps, step, 0)

    for u in range(subs):
        with jax.named_scope("opp"):
            for h in range(2):
                forward_last(h, u).wait_recv()
                sib_last(h, u).start()
        if u == 0:
            pt[...] = jnp.zeros((subs, kd, 2 * SUB), jnp.float32)
        with jax.named_scope("oppsib"):
            both = dyl.at[pl.ds(0, SUB)]
            remote(both, both, s_last, q_slast.at[u], r=sib).wait_recv()

        def dx_tile(t, _):
            cols = at(t * TILE, TILE)
            rhs = jnp.concatenate([dyl[pl.ds(u * SUB, SUB), cols], dyl[pl.ds(ROWS + u * SUB, SUB), cols]], axis=0)
            pt[u] += lax.dot_general(wv[:, cols], rhs, (((1,), (1,)), ((), ())), preferred_element_type=jnp.float32)
            return 0

        with jax.named_scope("dx"):
            lax.fori_loop(0, nb // TILE, dx_tile, 0)
        if u == subs - 1:
            dw_tiles(dyl, opp, runs, sibopp, runs, 0, 1)
        exchange_last(u)
        if u == 0:
            for old in range(MORE, THEN):
                deliver_early(jnp.int32(old))
            with jax.named_scope("reduce"):
                sum_step(steps - 1)

    deliver_late(steps - 1)
    for old in range(THEN, early):
        deliver_early(jnp.int32(old))
    with jax.named_scope("dw"):
        dw_tiles(dyl, opp, runs, sibopp, runs, 1, nb // TILE)
    for u in range(subs - 1):
        with jax.named_scope("reduce"):
            sum_last(u)
        deliver_last(u)

    for d in range(2):
        remote(dy, dyg.at[r], s_own.at[d], q_left.at[0], r=right).wait_send()
        remote(dyg.at[r, :, pl.ds(0, half)], dyg.at[r, :, pl.ds(0, half)], s_fwd.at[d], q_left.at[0], r=right).wait_send()
    for kind in range(3):
        remote(dy, dyg.at[r], s_sib.at[kind], q_left.at[0], r=right).wait_send()
    sent = dyg.at[r, pl.ds(0, runs * ROWS)]
    remote(sent, sent, s_opp, q_left.at[0], r=right).wait_send()
    sent = dyl.at[pl.ds(0, ROWS)]
    remote(sent, sent, s_last, q_left.at[0], r=right).wait_send()
    for sent in (spread, cross, gather):
        sent.wait_send()
    for s in range(steps - 3, steps):
        exchanged(s).wait_send()
    with jax.named_scope("reduce"):
        sum_last(subs - 1)
    for u in range(subs):
        exchanged_last(u).wait_send()
    deliver_last(subs - 1)

    facing = lax.rem(i - j + nc, nc) == nc // 2
    with jax.named_scope("dxfinal"):
        for kk in range(2):
            own = (i == j) & (k == kk)

            @pl.when(own)
            def _():
                rest = dxb.at[pl.ds(0, kd - kq)]
                remote(rest, rest, s_dx.at[0], q_dx.at[kk], c=i, r=sib).wait_recv()

            @pl.when(facing)
            def _():
                rest = dxb.at[pl.ds(0, kd), pl.ds(0, runs * ROWS)]
                remote(rest, rest, s_dx.at[0], q_dx.at[kk], c=i, r=sib).wait_recv()
                rest = dxl.at[pl.ds(0, kd)]
                remote(rest, rest, s_dx.at[0], q_dxl.at[kk], c=i, r=sib).wait_recv()

            @pl.when(jnp.logical_not(own | facing))
            def _():
                rest = dxb.at[pl.ds(0, kd)]
                remote(rest, rest, s_dx.at[0], q_dx.at[kk], c=i, r=sib).wait_recv()

    with jax.named_scope("drain"):
        @pl.when(i != j)
        def _():
            away = st.at[pl.ds(0, nbig)]
            remote(away, away, s_dx.at[0], q_dx.at[0], c=i, r=sib).wait_send()

        away = st.at[pl.ds(0, early - nbig + runs + subs * 2 * 2 * SUB // m)]
        remote(away, away, s_dx.at[1], q_dx.at[0], c=i, r=sib).wait_send()


def _store(nc, dwv, dxb, dxl, dx, dw, dxo, sem):
    kd = dwv.shape[0]
    tb = dxb.shape[1]
    puts = []
    for p in range(PUTS):
        rows = pl.ds(p * (kd // PUTS), kd // PUTS)
        puts.append(pltpu.make_async_copy(dwv.at[rows], dw.at[rows], sem.at[p]))
    for put in puts:
        put.start()
    r = lax.axis_index("r")
    i, k = r // 2, lax.rem(r, 2)
    facing = lax.rem(i - lax.axis_index("c") + nc, nc) == nc // 2
    dxo[:tb - ROWS] = dxb[:, :tb - ROWS].T
    for kk in range(2):
        rows = pl.ds(kk * kd, kd)
        runs = [dxl[rows, u * 2 * SUB:(u + 1) * 2 * SUB] for u in range(ROWS // SUB)]
        a = jnp.concatenate([run[:, :SUB] for run in runs], axis=1)
        b = jnp.concatenate([run[:, SUB:] for run in runs], axis=1)
        late = jnp.where(facing, jnp.where(k == kk, a, b), dxb[rows, tb - ROWS:])
        dxo[tb - ROWS:, kk * kd:(kk + 1) * kd] = late.T
    puts.append(pltpu.make_async_copy(dxo, dx, sem.at[PUTS]))
    puts[-1].start()
    for put in puts:
        put.wait()


def solution(mesh):
    nr, nc = mesh.shape["r"], mesh.shape["c"]

    def local(x, w, dy):
        tb, kb = x.shape
        kd, nb = w.shape
        m = 2 * ROWS
        nbig, runs, subs = tb // m, tb // ROWS - 1, ROWS // SUB
        nsteps = 6 * nbig + runs
        kq = kd // nc
        bf16, f32 = jnp.bfloat16, jnp.float32
        dma = pltpu.SemaphoreType.DMA
        any_ = pl.BlockSpec(memory_space=pl.ANY)
        vmem = pl.BlockSpec(memory_space=pltpu.VMEM)
        outs = kd * nb * 4 + kb * (tb + 2 * ROWS) * 2
        dwv, dxb, dxl, _ = pl.pallas_call(
            functools.partial(_main, nr, nc),
            name="linear_backward",
            out_shape=(pltpu.VMEM((kd, nb), f32), pltpu.VMEM((kb, tb), bf16),
                       pltpu.VMEM((kb, 2 * ROWS), bf16), jax.ShapeDtypeStruct((nr, tb, nb), bf16)),
            in_specs=[any_] * 3,
            out_specs=(vmem, vmem, vmem, any_),
            scratch_shapes=[
                pltpu.VMEM((2, m, nb), bf16), pltpu.VMEM((m, nb), bf16), pltpu.VMEM((kd, nb), bf16),
                pltpu.VMEM((tb, kb), bf16), pltpu.VMEM((kb, tb), bf16), pltpu.VMEM((nc, 2, kd // nc, tb), bf16),
                pltpu.VMEM((nr, kd, tb), bf16), pltpu.VMEM((3, kd, m), f32), pltpu.VMEM((subs, kd, 2 * SUB), f32),
                pltpu.VMEM((nc - 1, nsteps, kq, m), f32), pltpu.VMEM((nc - 1, subs, kq, 2 * SUB), f32),
                pltpu.VMEM((nsteps, kq, m), bf16), pltpu.VMEM((subs, kq, 2 * SUB), bf16),
                dma((2,)), dma((2,)), dma((3,)), dma, dma((nbig,)), dma((nbig,)), dma((3, nbig)),
                dma((2, runs)), dma((runs,)), dma, dma((2, subs)), dma((subs,)),
                dma((3,)), dma((3,)), dma((3 + subs,)), dma((nsteps + subs,)), dma((2,)), dma((2,)), dma((2,)), dma((4,)),
            ],
            compiler_params=pltpu.CompilerParams(collective_id=0, has_side_effects=True,
                                                 vmem_limit_bytes=VMEM - outs - 2**21),
        )(x, w, dy)
        return pl.pallas_call(
            functools.partial(_store, nc),
            name="store",
            out_shape=(jax.ShapeDtypeStruct((tb, kb), bf16), jax.ShapeDtypeStruct((kd, nb), f32)),
            in_specs=[vmem] * 3,
            out_specs=(any_, any_),
            scratch_shapes=[pltpu.VMEM((tb, kb), bf16), dma((PUTS + 1,))],
            compiler_params=pltpu.CompilerParams(vmem_limit_bytes=2**22),
        )(dwv, dxb, dxl)

    act = P(("dp", "r"), "c")
    return jax.shard_map(local, mesh=mesh, in_specs=(act, P("r", "c"), act),
                         out_specs=(act, act), check_vma=False)
```
